32 devices in a mesh: expert: 4 (over x, core), shard: 8 (over z, y).
Axes of the slice: x: 2, y: 2, z: 4, core: 2. Of those that a mesh axis runs over, the one named last changes fastest.
Arguments:
- master_gate: float32 [128, 2048, 768], P('expert', 'shard'), may hold values from -0.125 to 0.125
- master_up: float32 [128, 2048, 768], P('expert', 'shard'), may hold values from -0.125 to 0.125
- router_weight: float32 [2048, 128], P('shard', 'expert'), may hold values from -0.125 to 0.125
- router_gain: float32 [2048], P('shard'), may hold values from 0.25 to 1.75
Outputs:
- final_gate: bfloat16 [128, 768, 2048], P('expert', 'shard')
- final_up: bfloat16 [128, 768, 2048], P('expert', 'shard')
- serve_router: bfloat16 [2048, 128], replicated
The draws below stay inside these ranges and needn't reach their ends.
All inputs are finite; a program needn't handle non-finite values.
Results may differ from the reference program's by a relative error of at most 0.001.
Values may be sent and summed in bfloat16 or wider, within the bound.
A program may use at most 192 MiB of HBM per device.

```python
import jax
import jax.numpy as jnp

EXPERTS = 128
D_MODEL = 2048
D_EXPERT = 768


def shard_levels(key, extent, shards, least, largest):
    gain, own = 1.0, jax.random.fold_in(key, 6)
    for axis_at, shards_of in shards:
        heights = jnp.exp(jax.random.uniform(jax.random.fold_in(own, axis_at), (shards_of,), jnp.float32, least / len(shards), largest / len(shards)))
        gain = gain * jnp.repeat(heights, extent[axis_at] // shards_of).reshape([-1 if axis == axis_at else 1 for axis in range(len(extent))])
    return gain


def centred(key, extent, width, most, split=(), dtype=jnp.bfloat16):
    array = width * jax.random.normal(key, extent, jnp.float32)
    if split:
        array = array * shard_levels(key, extent, split, -0.22, 0.18)
    return jnp.clip(array, -most, most).astype(dtype)


def setup_inputs(seed: int = 0) -> dict:
    key_list = jax.random.split(jax.random.key(seed), 5)
    master_gate = centred(key_list[0], (EXPERTS, D_MODEL, D_EXPERT), D_MODEL ** -0.5, 0.125, ((0, 4), (1, 8)), jnp.float32)
    master_up = centred(key_list[1], (EXPERTS, D_MODEL, D_EXPERT), D_MODEL ** -0.5, 0.125, ((0, 4), (1, 8)), jnp.float32)
    router_weight = centred(key_list[2], (D_MODEL, EXPERTS), D_MODEL ** -0.5, 0.125, ((0, 8), (1, 4)), jnp.float32)
    router_gain = jnp.clip(1.0 + 0.15 * jax.random.normal(key_list[3], (D_MODEL,), jnp.float32), 0.25, 1.75)
    return {"master_gate": master_gate, "master_up": master_up, "router_weight": router_weight, "router_gain": router_gain}


def reference(master_gate, master_up, router_weight, router_gain):
    final_gate = master_gate.astype(jnp.bfloat16)
    final_gate = jnp.transpose(final_gate, (0, 2, 1))
    final_up = master_up.astype(jnp.bfloat16)
    final_up = jnp.transpose(final_up, (0, 2, 1))
    serve_router = (router_weight * router_gain[:, None]).astype(jnp.bfloat16)
    return final_gate, final_up, serve_router
```

```python
import functools

import jax
import jax.numpy as jnp
from jax import lax
from jax.experimental import pallas as pl
from jax.experimental.pallas import tpu as pltpu
from jax.sharding import PartitionSpec as P

NEAR = 1
PAIR = 2
CHUNK = 2
SLOTS = 4
LIMIT = 32


def plain(master_gate, master_up, router_weight, router_gain):
    narrow_gate, narrow_up = (master_gate.astype(jnp.bfloat16), master_up.astype(jnp.bfloat16))
    final_gate, final_up = (
        lax.all_to_all(narrow_gate, "shard", split_axis=2, concat_axis=1, tiled=True),
        lax.all_to_all(narrow_up, "shard", split_axis=2, concat_axis=1, tiled=True),
    )
    final_gate = jnp.transpose(final_gate, (0, 2, 1))
    final_up = jnp.transpose(final_up, (0, 2, 1))
    part_router = (router_weight * router_gain[:, None]).astype(jnp.bfloat16)
    row_router = lax.all_gather(part_router, "shard", axis=0, tiled=True)
    serve_router = lax.all_gather(row_router, "expert", axis=1, tiled=True)
    return (final_gate, final_up, serve_router)


def kernel(
    shards, groups, gate, up, weight, gain, out_gate, out_up, out_router,
    held, coming, router, load_sem, own_sem, send_sem, recv_sem,
    row_send, row_recv, column_send, column_recv,
):
    me, group = lax.axis_index("shard"), lax.axis_index("expert")
    _, _, experts, rows, depth = held.shape
    width = weight.shape[0]
    chunks = experts // CHUNK
    sources, outs = (gate, up), (out_gate, out_up)
    mine = pl.ds(pl.multiple_of(me * depth, depth), depth)
    my_part = pl.ds(pl.multiple_of(group * width, width), width)

    barrier = pltpu.get_barrier_semaphore()
    for step in range(1, shards):
        pl.semaphore_signal(barrier, inc=1, device_id={"shard": lax.rem(me + step, shards)})
    for step in range(1, groups):
        pl.semaphore_signal(barrier, inc=1, device_id={"expert": lax.rem(group + step, groups)})

    def load(which, expert):
        slot = lax.rem(expert, SLOTS)
        return pltpu.make_async_copy(sources[which].at[expert], coming.at[slot], load_sem.at[slot])

    def own(which, span):
        return pltpu.make_async_copy(
            held.at[which, me, span], outs[which].at[span, :, mine], own_sem.at[which]
        )

    def send(which, peer, span):
        return pltpu.make_async_remote_copy(
            src_ref=held.at[which, peer, span],
            dst_ref=outs[which].at[span, :, mine],
            send_sem=send_sem.at[which, peer],
            recv_sem=recv_sem.at[which, me],
            device_id={"shard": peer},
        )

    def arrival(which, peer):
        there = pl.ds(pl.multiple_of(peer * depth, depth), depth)
        return pltpu.make_async_remote_copy(
            src_ref=held.at[which, peer],
            dst_ref=outs[which].at[:, :, there],
            send_sem=send_sem.at[which, peer],
            recv_sem=recv_sem.at[which, peer],
            device_id={"shard": peer},
        )

    def row(peer):
        return pltpu.make_async_remote_copy(
            src_ref=router.at[me, my_part],
            dst_ref=router.at[me, my_part],
            send_sem=row_send.at[peer],
            recv_sem=row_recv.at[me],
            device_id={"shard": peer},
        )

    def row_arrival(peer):
        return pltpu.make_async_remote_copy(
            src_ref=router.at[peer, my_part],
            dst_ref=router.at[peer, my_part],
            send_sem=row_send.at[peer],
            recv_sem=row_recv.at[peer],
            device_id={"shard": peer},
        )

    def column(peer, of):
        part = pl.ds(pl.multiple_of(of * width, width), width)
        return pltpu.make_async_remote_copy(
            src_ref=router.at[:, part],
            dst_ref=router.at[:, part],
            send_sem=column_send.at[peer],
            recv_sem=column_recv.at[of],
            device_id={"expert": peer},
        )

    def to_peers(least, most, act):
        place, side = me // PAIR, lax.rem(me, PAIR)
        for away in range(least, most + 1):
            for turned in range(0 if away else 1, PAIR):
                other = lax.rem(side + turned, PAIR)
                if away == 0:
                    act(place * PAIR + other)
                    continue

                @pl.when(place + away < shards // PAIR)
                def _():
                    act((place + away) * PAIR + other)

                @pl.when(place >= away)
                def _():
                    act((place - away) * PAIR + other)

    last = shards // PAIR - 1
    for first in range(SLOTS):
        load(0, first).start()
    router[me, my_part] = (weight[...] * gain[...]).astype(jnp.bfloat16)

    def turn(which, expert):
        load(which, expert).wait()
        block = coming[lax.rem(expert, SLOTS)].T.astype(jnp.bfloat16)
        for peer in range(shards):
            held[which, peer, expert] = block[peer * rows:(peer + 1) * rows]

        @pl.when(expert + SLOTS < experts)
        def _():
            load(which, expert + SLOTS).start()

    def turns(which, chunk):
        @pl.loop(0, CHUNK)
        def _(step):
            turn(which, chunk * CHUNK + step)

    def near(which, chunk):
        span = pl.ds(chunk * CHUNK, CHUNK)
        to_peers(0, NEAR, lambda peer: send(which, peer, span).start())
        own(which, span).start()

    for which in range(2):
        turns(which, 0)
        if which == 0:
            pl.semaphore_wait(barrier, shards + groups - 2)
            to_peers(0, last, lambda peer: row(peer).start())
        else:
            near(0, chunks - 1)

        @pl.loop(1, chunks)
        def _(chunk):
            turns(which, chunk)
            near(which, chunk - 1)

        if which == 0:
            for first in range(SLOTS):
                load(1, first).start()
    near(1, chunks - 1)
    whole = pl.ds(0, experts)
    for away in range(NEAR + 1, last + 1):
        for which in range(2):
            to_peers(away, away, lambda peer: send(which, peer, whole).start())

    to_peers(0, last, lambda peer: row_arrival(peer).wait_recv())
    for step in range(1, groups):
        column(lax.rem(group + step, groups), group).start()
    for step in range(1, groups):
        peer = lax.rem(group + step, groups)
        column(peer, peer).wait_recv()
    for shard in range(shards):
        out_router[shard * depth:(shard + 1) * depth] = router[shard].T
    to_peers(0, last, lambda peer: row(peer).wait_send())
    for step in range(1, groups):
        column(lax.rem(group + step, groups), group).wait_send()

    for which in range(2):
        own(which, whole).wait()
        to_peers(0, last, lambda peer: arrival(which, peer).wait())


def put_out(gate, up, router, out_gate, out_up, out_router, sem):
    copies = [
        pltpu.make_async_copy(source, out, sem.at[at])
        for at, (source, out) in enumerate(((gate, out_gate), (up, out_up), (router, out_router)))
    ]
    for copy in copies:
        copy.start()
    for copy in copies:
        copy.wait()


def per_device(shards, groups, master_gate, master_up, router_weight, router_gain):
    experts, depth, inner = master_gate.shape
    width = router_weight.shape[1]
    rows = inner // shards
    if shards % PAIR or depth % 128 or rows % 16 or width % 16 or experts % CHUNK or experts < 2 * CHUNK or (width * groups) % 128:
        return plain(master_gate, master_up, router_weight, router_gain)
    anywhere = pl.BlockSpec(memory_space=pl.ANY)
    inside = pl.BlockSpec(memory_space=pltpu.VMEM)
    final = pltpu.VMEM((experts, rows, shards * depth), jnp.bfloat16)
    dma = pltpu.SemaphoreType.DMA
    kept = pl.pallas_call(
        functools.partial(kernel, shards, groups),
        out_shape=(final, final, pltpu.VMEM((shards * depth, groups * width), jnp.bfloat16)),
        in_specs=[anywhere, anywhere, inside, inside],
        out_specs=(inside, inside, inside),
        scratch_shapes=[
            pltpu.VMEM((2, shards, experts, rows, depth), jnp.bfloat16),
            pltpu.VMEM((SLOTS, depth, inner), jnp.float32),
            pltpu.VMEM((shards, groups * width, depth), jnp.bfloat16),
            dma((SLOTS,)), dma((2,)), dma((2, shards)), dma((2, shards)),
            dma((shards,)), dma((shards,)), dma((groups,)), dma((groups,)),
        ],
        compiler_params=pltpu.CompilerParams(
            collective_id=0, has_side_effects=True, vmem_limit_bytes=LIMIT * 2**20
        ),
    )(master_gate, master_up, router_weight.T, router_gain[None])
    return pl.pallas_call(
        put_out,
        out_shape=tuple(jax.ShapeDtypeStruct(array.shape, array.dtype) for array in kept),
        in_specs=[inside] * 3,
        out_specs=(anywhere,) * 3,
        scratch_shapes=[dma((3,))],
        compiler_params=pltpu.CompilerParams(vmem_limit_bytes=2**20),
    )(*kept)


def solution(mesh):
    placed = (
        P("expert", "shard", None),
        P("expert", "shard", None),
        P("shard", "expert"),
        P("shard"),
    )
    return jax.shard_map(
        functools.partial(per_device, mesh.shape["shard"], mesh.shape["expert"]),
        mesh=mesh,
        in_specs=placed,
        out_specs=(P("expert", "shard", None), P("expert", "shard", None), P()),
        check_vma=False,
    )
```
